32 devices in a mesh: gx: 4 (over y, x), gy: 2 (over core), gz: 4 (over z).
Axes of the slice: x: 2, y: 2, z: 4, core: 2. Of those that a mesh axis runs over, the one named last changes fastest.
Arguments:
- star_residual: bfloat16 [128, 64, 1152], P(('gx', 'gy', 'gz')), may hold values from -6 to 6
- patch_inverse: bfloat16 [128, 1152, 1152], P(('gx', 'gy', 'gz')), may hold values from -0.1875 to 0.1875
- block_owner: int32 [128, 9], P(('gx', 'gy', 'gz')), may hold values from 0 to 31, as said below
- block_slot: int32 [128, 9], P(('gx', 'gy', 'gz')), may hold values from 0 to 1, as said below
- recv_target: int32 [32, 27, 2], P(('gx', 'gy', 'gz')), may hold values from -1 to 7, as said below
Outputs:
- owned_sum: float32 [256, 64, 128], P(('gx', 'gy', 'gz'))
- combined: float32 [128, 9, 64, 128], P(('gx', 'gy', 'gz'))
The draws below stay inside these ranges and needn't reach their ends.
Inputs may be any that keep to these rules, and one draw needn't show every extreme that they name: `block_owner`: each block's owner is the block's own partition or one whose coordinate differs by at most one step along each of the three mesh axes, counted with wrap-around. `block_slot`: blocks of one partition that have the same owner have distinct slots; in every partition some owner receives exactly 2 of its blocks. `recv_target`: every slot that a block uses maps to an owned block of its owner; slots that no block uses hold -1.
All inputs are finite; a program needn't handle non-finite values.
Results may differ from the reference program's by a relative error of at most 0.0003.
Values sent between devices are 32-bit elements; how exact they have to be, the bound alone decides.
A program may use at most 64 MiB of HBM per device.

```python
import jax
import jax.numpy as jnp
from jax import lax

BW = 128
PDOF = 1152
PATCH_DEV = 4
RHS = 64
OWNB = 8
CAP = 2
NBLK = 9
PX = 4
PY = 2
PZ = 4
NDEV = 32
PATCHES = 128


def axis_deltas(extent):
    if extent == 1:
        return [0]
    if extent == 2:
        return [0, 1]
    return [-1, 0, 1]


def routing(key):
    offsets = [(a, b, c) for a in axis_deltas(PX) for b in axis_deltas(PY) for c in axis_deltas(PZ)]
    offset_total = len(offsets)
    step_x = jnp.array([o[0] for o in offsets], jnp.int32)
    step_y = jnp.array([o[1] for o in offsets], jnp.int32)
    step_z = jnp.array([o[2] for o in offsets], jnp.int32)
    codes = jnp.array([9 * (o[0] + 1) + 3 * (o[1] + 1) + (o[2] + 1) for o in offsets], jnp.int32)
    block_total = PATCH_DEV * NBLK
    base = jax.random.fold_in(key, 1301)

    def single(device):
        device_key = jax.random.fold_in(base, device)
        key_fav, key_score, key_assign = jax.random.split(device_key, 3)
        favored = jax.random.randint(key_fav, (), 0, offset_total)
        pairs = jnp.arange(offset_total * CAP, dtype=jnp.int32)
        scores = jax.random.permutation(key_score, offset_total * CAP).astype(jnp.int32)
        scores = jnp.where(pairs // CAP == favored, scores - offset_total * CAP, scores)
        ranked = jnp.argsort(scores, stable=True).astype(jnp.int32)
        chosen = ranked[:block_total]
        picked = chosen[jax.random.permutation(key_assign, block_total).astype(jnp.int32)]
        offset_ids = picked // CAP
        slot_ids = (picked % CAP).astype(jnp.int32)
        coord_x = device // (PY * PZ)
        coord_y = device // PZ % PY
        coord_z = device % PZ
        owner_ids = ((coord_x + step_x[offset_ids]) % PX * PY * PZ + (coord_y + step_y[offset_ids]) % PY * PZ + (coord_z + step_z[offset_ids]) % PZ).astype(jnp.int32)
        return (owner_ids, slot_ids, codes[offset_ids])
    owner_all, slot_all, code_all = jax.vmap(single)(jnp.arange(NDEV, dtype=jnp.int32))
    target_all = jax.random.randint(jax.random.fold_in(key, 2417), (NDEV, block_total), 0, OWNB).astype(jnp.int32)
    index_all = (owner_all * 27 * CAP + code_all * CAP + slot_all).reshape(-1)
    target_table = jnp.full((NDEV * 27 * CAP,), -1, jnp.int32).at[index_all].set(target_all.reshape(-1))
    return (owner_all.reshape(NDEV * PATCH_DEV, NBLK), slot_all.reshape(NDEV * PATCH_DEV, NBLK), target_table.reshape(NDEV, 27, CAP))


def draw_block_owner(key, part):
    return routing(key)[0]


def draw_block_slot(key, part):
    return routing(key)[1]


def draw_recv_target(key, part):
    return routing(key)[2]


def block_levels(key, shape, shards, least, top_value):
    loudness, own = 1.0, jax.random.fold_in(key, 6)
    for axis_at, shards_of in shards:
        heights = jnp.exp(jax.random.uniform(jax.random.fold_in(own, axis_at), (shards_of,), jnp.float32, least / len(shards), top_value / len(shards)))
        loudness = loudness * jnp.repeat(heights, shape[axis_at] // shards_of).reshape([-1 if axis == axis_at else 1 for axis in range(len(shape))])
    return loudness


def noise(own_key, dims, width, most, cuts=(), held_as=jnp.bfloat16):
    loudness = block_levels(own_key, dims, cuts, -0.22, 0.18) if cuts else 1.0
    values = jax.random.normal(own_key, dims, jnp.float32) * width * loudness
    return jnp.minimum(jnp.maximum(values, -most), most).astype(held_as)


def setup_inputs(seed: int = 0) -> dict:
    seeds = jax.random.split(jax.random.key(seed), 6)
    star_residual = noise(seeds[0], (PATCHES, RHS, PDOF), 1.0, 6.0, ((0, 32),))
    patch_inverse = noise(seeds[1], (PATCHES, PDOF, PDOF), PDOF ** -0.5, 0.1875, ((0, 32),))
    block_owner = draw_block_owner(jax.random.fold_in(seeds[5], 71), 0)
    block_slot = draw_block_slot(jax.random.fold_in(seeds[5], 71), 0)
    recv_target = draw_recv_target(jax.random.fold_in(seeds[5], 71), 0)
    return dict(star_residual=star_residual, patch_inverse=patch_inverse, block_owner=block_owner, block_slot=block_slot, recv_target=recv_target)


def axis_code(far_index, near_index, extent):
    distance = (far_index - near_index) % extent
    return jnp.where(distance == 0, 1, jnp.where(distance == 1, 2, 0)).astype(jnp.int32)


def offset_code(owner_ids, sender_ids):
    owner_x = owner_ids // (PY * PZ)
    owner_y = (owner_ids // PZ) % PY
    owner_z = owner_ids % PZ
    sender_x = sender_ids // (PY * PZ)
    sender_y = (sender_ids // PZ) % PY
    sender_z = sender_ids % PZ
    return (9 * axis_code(owner_x, sender_x, PX) + 3 * axis_code(owner_y, sender_y, PY)
            + axis_code(owner_z, sender_z, PZ)).astype(jnp.int32)


def reference(star_residual, patch_inverse, block_owner, block_slot, recv_target):
    residual_wide = star_residual.astype(jnp.float32)
    inverse_wide = patch_inverse.astype(jnp.float32).reshape(PATCHES, NBLK, BW, PDOF)
    contribution = jnp.einsum('prj,pbwj->pbrw', residual_wide, inverse_wide, precision=lax.Precision.HIGHEST)
    blocks = contribution.reshape(PATCHES * NBLK, RHS, BW)
    sender_ids = (jnp.arange(PATCHES * NBLK, dtype=jnp.int32) // (PATCH_DEV * NBLK)).astype(jnp.int32)
    owner_ids = block_owner.reshape(-1).astype(jnp.int32)
    slot_ids = block_slot.reshape(-1).astype(jnp.int32)
    codes = offset_code(owner_ids, sender_ids)
    targets = recv_target[owner_ids, codes, slot_ids].astype(jnp.int32)
    keys = (owner_ids * OWNB + targets).astype(jnp.int32)
    owned_sum = jax.ops.segment_sum(blocks, keys, num_segments=NDEV * OWNB)
    combined = owned_sum[keys].reshape(PATCHES, NBLK, RHS, BW)
    return owned_sum, combined
```

```python
import functools

import jax
import jax.numpy as jnp
from jax import lax
from jax.experimental import pallas as pl
from jax.experimental.pallas import tpu as pltpu
from jax.sharding import PartitionSpec as P

OWNB = 8
CHUNKS = 2
MESH = pl.DeviceIdType.MESH


def offsets(extent):
    return [0, 1, -1][: min(extent, 3)]


def offset_index(far, near, extent):
    distance = (far - near) % extent
    return jnp.where(distance <= 1, distance, 2).astype(jnp.int32)


def code_of(offset):
    return offset + 1


def kernel(cfg, src_ref, key_ref, table_ref, star_ref, inv_hbm, owned_ref, comb_ref,
           star, inv, sent, came, tgt_out, tgt, pd, px, ry, rx, own, g1, g2, ans, back,
           load_sem, tgt_send, tgt_recv, a_send, a_recv, y_send, y_recv, x_send, x_recv,
           g_send, g_recv, h_send, h_recv, b_send, b_recv):
    nx, ny, nz, chunks, block_count, capacity = cfg
    gx, gy, gz = lax.axis_index("gx"), lax.axis_index("gy"), lax.axis_index("gz")
    patch_count = inv_hbm.shape[0] // block_count
    total = inv_hbm.shape[0]
    rows = came.shape[2]
    lanes = came.shape[3]
    pairs = [(dy, dz) for dy in offsets(ny) for dz in offsets(nz)]
    count = len(pairs)
    far = sorted(range(1, count), key=lambda q: pairs[q][1] == 0)
    near_x = (gx + 1 - 2 * (gx % 2), gy, gz)
    near_y = ((gx + 2) % 4, gy, gz)
    corner = (3 - gx, gy, gz)

    def ahead(q):
        return (gx, (gy + pairs[q][0] + ny) % ny, (gz + pairs[q][1] + nz) % nz)

    def behind(q):
        return (gx, (gy - pairs[q][0] + ny) % ny, (gz - pairs[q][1] + nz) % nz)

    loads = [pltpu.make_async_copy(star_ref, star, load_sem.at[patch_count])]
    for p in range(patch_count):
        part = pl.ds(p * block_count, block_count)
        loads.append(pltpu.make_async_copy(inv_hbm.at[part], inv.at[part], load_sem.at[p]))
    for load in loads:
        load.start()

    barrier = pltpu.get_barrier_semaphore()
    greeted = [ahead(q) for q in range(1, count)] + [near_x, near_y, corner]
    for device in greeted:
        pl.semaphore_signal(barrier, inc=1, device_id=device, device_id_type=MESH)

    parity = gx % 2
    for role in range(3):
        code_x = (1, 2 * parity, 2 - 2 * parity)[role]
        held = tgt if role == 0 else tgt_out
        for q in range(count):
            code = 9 * code_x + 3 * code_of(pairs[q][0]) + code_of(pairs[q][1])
            for s in range(capacity):
                i = q * capacity + s
                held[role, i:i + 1, :] = jnp.full((1, lanes), table_ref[0, code, s], jnp.int32)

    pl.semaphore_wait(barrier, len(greeted))

    sends = []

    def remote(source, target, send_sem, recv_sem, device):
        copy = pltpu.make_async_remote_copy(
            src_ref=source, dst_ref=target, send_sem=send_sem, recv_sem=recv_sem,
            device_id=device, device_id_type=MESH)
        return copy

    def launch(copy):
        copy.start()
        sends.append(copy)
        return copy

    tgt_copies = {}
    for role, device in ((1, near_x), (2, corner)):
        tgt_copies[role] = launch(remote(
            tgt_out.at[role], tgt.at[role], tgt_send.at[role - 1], tgt_recv.at[role - 1], device))

    def slot(q, role):
        return (q * 3 + role) * capacity

    def part(ref, c, q, role):
        return ref.at[c, pl.ds(slot(q, role), capacity)]

    for load in loads:
        load.wait()

    a_copies = {}
    for role in (2, 1, 0):
        for q in far + [0]:
            held = came if q == 0 else sent
            for s in range(capacity):
                k = slot(q, role) + s
                n = src_ref[k]
                block = lax.dot_general(
                    star[n // block_count], inv[n], (((1,), (1,)), ((), ())),
                    preferred_element_type=jnp.float32)
                for c in range(chunks):
                    held[c, k] = block[c * rows:(c + 1) * rows]
            if q:
                a_copies[q, role, 0] = launch(remote(
                    part(sent, 0, q, role), part(came, 0, q, role),
                    a_send.at[q, role, 0], a_recv.at[q, role, 0], ahead(q)))
        for c in range(1, chunks):
            for q in far:
                a_copies[q, role, c] = launch(remote(
                    part(sent, c, q, role), part(came, c, q, role),
                    a_send.at[q, role, c], a_recv.at[q, role, c], ahead(q)))

    tgt_copies[1].wait_recv()
    tgt_copies[2].wait_recv()

    def targets(role, i):
        return jnp.broadcast_to(tgt[role, i:i + 1, :], (8, lanes))

    def reduce(role, c, store):
        for q in far:
            a_copies[q, role, c].wait_recv()

        def body(r, carry):
            at = pl.ds(pl.multiple_of(r * 8, 8), 8)
            sums = [jnp.zeros((8, lanes), jnp.float32) for _ in range(OWNB)]
            for q in range(count):
                for s in range(capacity):
                    value = came[c, slot(q, role) + s, at, :]
                    where = targets(role, q * capacity + s)
                    for t in range(OWNB):
                        sums[t] = sums[t] + jnp.where(where == t, value, 0.0)
            for t in range(OWNB):
                store(t, at, r, sums[t])
            return carry

        lax.fori_loop(0, rows // 8, body, 0)

    b_copies = {}

    def answer(role, c, held):
        def body(r, carry):
            at = pl.ds(pl.multiple_of(r * 8, 8), 8)
            values = [held[c, t, at, :] for t in range(OWNB)]
            for q in range(count):
                to = back if q == 0 else ans
                for s in range(capacity):
                    where = targets(role, q * capacity + s)
                    out = values[0]
                    for t in range(1, OWNB):
                        out = jnp.where(where == t, values[t], out)
                    to[c, slot(q, role) + s, at, :] = out
            return carry

        lax.fori_loop(0, rows // 8, body, 0)
        for q in far:
            b_copies[q, role, c] = launch(remote(
                part(ans, c, q, role), part(back, c, q, role),
                b_send.at[q, role, c], b_recv.at[q, role, c], behind(q)))

    y_copies, x_copies, g_copies, h_copies = {}, {}, {}, {}

    def stage_corner(c):
        def store(t, at, r, value):
            pd[c, t, at, :] = value
        reduce(2, c, store)
        y_copies[c] = launch(remote(pd.at[c], ry.at[c], y_send.at[c], y_recv.at[c], near_y))

    def stage_near(c):
        y_copies[c].wait_recv()

        def store(t, at, r, value):
            px[c, t, at, :] = value + ry[c, t, at, :]
        reduce(1, c, store)
        x_copies[c] = launch(remote(px.at[c], rx.at[c], x_send.at[c], x_recv.at[c], near_x))

    def stage_own(c):
        x_copies[c].wait_recv()

        def store(t, at, r, value):
            value = value + rx[c, t, at, :]
            own[c, t, at, :] = value
            owned_ref[t, pl.ds(pl.multiple_of(c * rows + r * 8, 8), 8), :] = value
        reduce(0, c, store)
        g_copies[c] = launch(remote(own.at[c], g1.at[c], g_send.at[c], g_recv.at[c], near_x))
        answer(0, c, own)

    def stage_back_near(c):
        g_copies[c].wait_recv()
        h_copies[c] = launch(remote(g1.at[c], g2.at[c], h_send.at[c], h_recv.at[c], near_y))
        answer(1, c, g1)

    def stage_back_corner(c):
        h_copies[c].wait_recv()
        answer(2, c, g2)

    stages = [stage_corner, stage_near, stage_own, stage_back_near, stage_back_corner]
    steps = [(c + 2 * i, i, c) for i in range(len(stages)) for c in range(chunks)]
    for _, i, c in sorted(steps):
        stages[i](c)

    for copy in b_copies.values():
        copy.wait_recv()

    def gather(n, carry):
        k = key_ref[n]
        for c in range(chunks):
            comb_ref[n, c * rows:(c + 1) * rows, :] = back[c, k]
        return carry

    lax.fori_loop(0, total, gather, 0, unroll=4)
    for copy in sends:
        copy.wait_send()


def on_device(star_residual, patch_inverse, block_owner, block_slot, recv_target):
    nx, ny, nz = lax.axis_size("gx"), lax.axis_size("gy"), lax.axis_size("gz")
    gx, gy, gz = lax.axis_index("gx"), lax.axis_index("gy"), lax.axis_index("gz")
    patch_count, rhs_count, patch_order = star_residual.shape
    block_count = block_owner.shape[1]
    width = patch_order // block_count
    capacity = recv_target.shape[2]
    total = patch_count * block_count
    ly, lz = len(offsets(ny)), len(offsets(nz))
    count = ly * lz
    slots = count * 3 * capacity
    chunks = CHUNKS
    rows = rhs_count // chunks
    owner = block_owner.reshape(-1)
    at_x = offset_index(owner // (ny * nz), gx, nx)
    role = jnp.where((at_x > 0) & (gx % 2 == 1), 3 - at_x, at_x)
    at_y = offset_index(owner // nz % ny, gy, ny)
    at_z = offset_index(owner % nz, gz, nz)
    key = ((at_y * lz + at_z) * 3 + role) * capacity + block_slot.reshape(-1)
    order = jnp.arange(total, dtype=jnp.int32)
    hit = key[None, :] == jnp.arange(slots, dtype=jnp.int32)[:, None]
    src = jnp.sum(jnp.where(hit, order[None, :], 0), axis=1).astype(jnp.int32)

    smem = pl.BlockSpec(memory_space=pltpu.SMEM)
    vmem = pl.BlockSpec(memory_space=pltpu.VMEM)
    anywhere = pl.BlockSpec(memory_space=pl.ANY)
    f32 = jnp.float32
    slotted = pltpu.VMEM((chunks, slots, rows, width), f32)
    targeted = pltpu.VMEM((chunks, OWNB, rows, width), f32)
    dma = pltpu.SemaphoreType.DMA
    owned, comb = pl.pallas_call(
        functools.partial(kernel, (nx, ny, nz, chunks, block_count, capacity)),
        out_shape=(
            jax.ShapeDtypeStruct((OWNB, rhs_count, width), f32),
            jax.ShapeDtypeStruct((total, rhs_count, width), f32),
        ),
        in_specs=[smem, smem, smem, anywhere, anywhere],
        out_specs=(vmem, vmem),
        scratch_shapes=[
            pltpu.VMEM(star_residual.shape, star_residual.dtype),
            pltpu.VMEM((total, width, patch_order), patch_inverse.dtype),
            slotted, slotted,
            pltpu.VMEM((3, count * capacity, width), jnp.int32),
            pltpu.VMEM((3, count * capacity, width), jnp.int32),
            targeted, targeted, targeted, targeted, targeted, targeted, targeted,
            slotted, slotted,
            dma((patch_count + 1,)), dma((2,)), dma((2,)),
            dma((count, 3, chunks)), dma((count, 3, chunks)),
            dma((chunks,)), dma((chunks,)), dma((chunks,)), dma((chunks,)),
            dma((chunks,)), dma((chunks,)), dma((chunks,)), dma((chunks,)),
            dma((count, 3, chunks)), dma((count, 3, chunks)),
        ],
        compiler_params=pltpu.CompilerParams(
            collective_id=0, has_side_effects=True, vmem_limit_bytes=56 * 1024 * 1024),
    )(src, key, recv_target, star_residual,
      patch_inverse.reshape(total, width, patch_order))
    return owned, comb.reshape(patch_count, block_count, rhs_count, width)


def solution(mesh):
    placed = (
        P(("gx", "gy", "gz"), None, None),
        P(("gx", "gy", "gz"), None, None),
        P(("gx", "gy", "gz"), None),
        P(("gx", "gy", "gz"), None),
        P(("gx", "gy", "gz"), None, None),
    )
    return jax.shard_map(
        on_device,
        mesh=mesh,
        in_specs=placed,
        out_specs=(P(("gx", "gy", "gz"), None, None), P(("gx", "gy", "gz"), None, None, None)),
        check_vma=False,
    )
```

```python
import functools

import jax
import jax.numpy as jnp
from jax import lax
from jax.experimental import pallas as pl
from jax.experimental.pallas import tpu as pltpu
from jax.sharding import PartitionSpec as P

OWNB = 8
CHUNKS = 2
MESH = pl.DeviceIdType.MESH


def offsets(extent):
    return [0, 1, -1][: min(extent, 3)]


def offset_index(far, near, extent):
    distance = lax.rem(far - near + extent, extent)
    return jnp.where(distance <= 1, distance, 2)


def slot_of(owner, block_slot, extents, capacity):
    nx, ny, nz = extents
    gx, gy, gz = lax.axis_index("gx"), lax.axis_index("gy"), lax.axis_index("gz")
    at_x = offset_index(lax.div(owner, ny * nz), gx, nx)
    role = jnp.where((at_x > 0) & (lax.rem(gx, 2) == 1), 3 - at_x, at_x)
    at_y = offset_index(lax.rem(lax.div(owner, nz), ny), gy, ny)
    at_z = offset_index(lax.rem(owner, nz), gz, nz)
    return ((at_y * len(offsets(nz)) + at_z) * 3 + role) * capacity + block_slot


def code_of(offset):
    return offset + 1


def gather_kernel(cfg, owner_ref, slot_ref, held_ref, back_ref, owned_ref, comb_ref,
                  own, comb, in_sem, out_sem):
    extents, capacity = cfg
    patch_count, block_count = owner_ref.shape
    own_in = pltpu.make_async_copy(held_ref, own, in_sem.at[patch_count])
    own_out = pltpu.make_async_copy(own, owned_ref, out_sem.at[patch_count])
    own_in.start()
    for p in range(patch_count):
        def fetch(b, carry):
            k = slot_of(owner_ref[p, b], slot_ref[p, b], extents, capacity)
            pltpu.make_async_copy(back_ref.at[k], comb.at[p, b], in_sem.at[p]).start()
            return carry
        lax.fori_loop(0, block_count, fetch, 0, unroll=True)
    own_in.wait()
    own_out.start()
    outs = [own_out]
    for p in range(patch_count):
        pltpu.make_async_copy(back_ref.at[pl.ds(0, block_count)], comb.at[p], in_sem.at[p]).wait()
        out = pltpu.make_async_copy(comb.at[p], comb_ref.at[p], out_sem.at[p])
        out.start()
        outs.append(out)
    for out in outs:
        out.wait()


def kernel(cfg, owner_ref, slot_ref, table_ref, star_ref, inv_hbm, owned_ref, back,
           star, inv, key_ref, src_ref, sent, came, tgt_out, tgt, pd, px, ry, rx, own, g1, g2, ans,
           own_sem, self_sem, load_sem, tgt_send, tgt_recv, a_send, a_recv, y_send, y_recv, x_send, x_recv,
           g_send, g_recv, h_send, h_recv, b_send, b_recv):
    nx, ny, nz, chunks, block_count, capacity = cfg
    gx, gy, gz = lax.axis_index("gx"), lax.axis_index("gy"), lax.axis_index("gz")
    patch_count = inv_hbm.shape[0] // block_count
    total = inv_hbm.shape[0]
    rows = came.shape[2]
    lanes = came.shape[3]
    pairs = [(dy, dz) for dy in offsets(ny) for dz in offsets(nz)]
    count = len(pairs)
    far = sorted(range(1, count), key=lambda q: pairs[q][1] == 0)
    near_x = (gx + 1 - 2 * (gx % 2), gy, gz)
    near_y = ((gx + 2) % 4, gy, gz)
    corner = (3 - gx, gy, gz)

    def ahead(q):
        return (gx, (gy + pairs[q][0] + ny) % ny, (gz + pairs[q][1] + nz) % nz)

    def behind(q):
        return (gx, (gy - pairs[q][0] + ny) % ny, (gz - pairs[q][1] + nz) % nz)

    loads = [pltpu.make_async_copy(star_ref, star, load_sem.at[patch_count])]
    for p in range(patch_count):
        part = pl.ds(p * block_count, block_count)
        loads.append(pltpu.make_async_copy(inv_hbm.at[part], inv.at[part], load_sem.at[p]))
    for load in loads:
        load.start()

    barrier = pltpu.get_barrier_semaphore()
    greeted = [ahead(q) for q in range(1, count)] + [near_x, near_y, corner]
    for device in greeted:
        pl.semaphore_signal(barrier, inc=1, device_id=device, device_id_type=MESH)

    parity = gx % 2
    for role in range(3):
        code_x = (1, 2 * parity, 2 - 2 * parity)[role]
        held = tgt if role == 0 else tgt_out
        for q in range(count):
            code = 9 * code_x + 3 * code_of(pairs[q][0]) + code_of(pairs[q][1])
            for s in range(capacity):
                i = q * capacity + s
                held[role, i:i + 1, :] = jnp.full((1, lanes), table_ref[0, s, code], jnp.int32)

    def number(n, carry):
        p, b = lax.div(n, block_count), lax.rem(n, block_count)
        key_ref[n] = slot_of(owner_ref[p, b], slot_ref[p, b], (nx, ny, nz), capacity)
        return carry

    lax.fori_loop(0, total, number, 0)

    def invert(k, carry):
        found = jnp.int32(0)
        for n in range(total):
            found = jnp.where(key_ref[n] == k, n, found)
        src_ref[k] = found
        return carry

    lax.fori_loop(0, count * 3 * capacity, invert, 0)

    pl.semaphore_wait(barrier, len(greeted))

    sends = []

    def remote(source, target, send_sem, recv_sem, device):
        copy = pltpu.make_async_remote_copy(
            src_ref=source, dst_ref=target, send_sem=send_sem, recv_sem=recv_sem,
            device_id=device, device_id_type=MESH)
        return copy

    def launch(copy):
        copy.start()
        sends.append(copy)
        return copy

    tgt_copies = {}
    for role, device in ((1, near_x), (2, corner)):
        tgt_copies[role] = launch(remote(
            tgt_out.at[role], tgt.at[role], tgt_send.at[role - 1], tgt_recv.at[role - 1], device))

    def slot(q, role):
        return (q * 3 + role) * capacity

    def part(ref, c, q, role):
        return ref.at[c, pl.ds(slot(q, role), capacity)]

    for load in loads:
        load.wait()

    a_copies = {}
    for role in (2, 1, 0):
        for q in far + [0]:
            held = came if q == 0 else sent
            for s in range(capacity):
                k = slot(q, role) + s
                n = src_ref[k]
                block = lax.dot_general(
                    star[n // block_count], inv[n], (((1,), (1,)), ((), ())),
                    preferred_element_type=jnp.float32)
                for c in range(chunks):
                    held[c, k] = block[c * rows:(c + 1) * rows]
            if q:
                a_copies[q, role, 0] = launch(remote(
                    part(sent, 0, q, role), part(came, 0, q, role),
                    a_send.at[q, role, 0], a_recv.at[q, role, 0], ahead(q)))
        for c in range(1, chunks):
            for q in far:
                a_copies[q, role, c] = launch(remote(
                    part(sent, c, q, role), part(came, c, q, role),
                    a_send.at[q, role, c], a_recv.at[q, role, c], ahead(q)))

    tgt_copies[1].wait_recv()
    tgt_copies[2].wait_recv()

    def targets(role, i):
        return jnp.broadcast_to(tgt[role, i:i + 1, :], (8, lanes))

    def reduce(role, c, store):
        for q in far:
            a_copies[q, role, c].wait_recv()

        def body(r, carry):
            at = pl.ds(pl.multiple_of(r * 8, 8), 8)
            sums = [jnp.zeros((8, lanes), jnp.float32) for _ in range(OWNB)]
            for q in range(count):
                for s in range(capacity):
                    value = came[c, slot(q, role) + s, at, :]
                    where = targets(role, q * capacity + s)
                    for t in range(OWNB):
                        sums[t] = sums[t] + jnp.where(where == t, value, 0.0)
            for t in range(OWNB):
                store(t, at, r, sums[t])
            return carry

        lax.fori_loop(0, rows // 8, body, 0)

    b_copies = {}
    locals_ = []

    def landing(c, q, role):
        return back.at[pl.ds(slot(q, role), capacity), pl.ds(c * rows, rows)]

    def put(source, target, sem):
        copy = pltpu.make_async_copy(source, target, sem)
        copy.start()
        locals_.append(copy)

    def answer(role, c, held):
        def body(r, carry):
            at = pl.ds(pl.multiple_of(r * 8, 8), 8)
            values = [held[c, t, at, :] for t in range(OWNB)]
            for q in range(count):
                for s in range(capacity):
                    where = targets(role, q * capacity + s)
                    out = values[0]
                    for t in range(1, OWNB):
                        out = jnp.where(where == t, values[t], out)
                    ans[c, slot(q, role) + s, at, :] = out
            return carry

        lax.fori_loop(0, rows // 8, body, 0)
        put(part(ans, c, 0, role), landing(c, 0, role), self_sem.at[role, c])
        for q in far:
            b_copies[q, role, c] = launch(remote(
                part(ans, c, q, role), landing(c, q, role),
                b_send.at[q, role, c], b_recv.at[q, role, c], behind(q)))

    y_copies, x_copies, g_copies, h_copies = {}, {}, {}, {}

    def stage_corner(c):
        def store(t, at, r, value):
            pd[c, t, at, :] = value
        reduce(2, c, store)
        y_copies[c] = launch(remote(pd.at[c], ry.at[c], y_send.at[c], y_recv.at[c], near_y))

    def stage_near(c):
        y_copies[c].wait_recv()

        def store(t, at, r, value):
            px[c, t, at, :] = value + ry[c, t, at, :]
        reduce(1, c, store)
        x_copies[c] = launch(remote(px.at[c], rx.at[c], x_send.at[c], x_recv.at[c], near_x))

    def stage_own(c):
        x_copies[c].wait_recv()

        def store(t, at, r, value):
            own[c, t, at, :] = value + rx[c, t, at, :]
        reduce(0, c, store)
        g_copies[c] = launch(remote(own.at[c], g1.at[c], g_send.at[c], g_recv.at[c], near_x))
        put(own.at[c], owned_ref.at[:, pl.ds(c * rows, rows)], own_sem.at[c])
        answer(0, c, own)

    def stage_back_near(c):
        g_copies[c].wait_recv()
        h_copies[c] = launch(remote(g1.at[c], g2.at[c], h_send.at[c], h_recv.at[c], near_y))
        answer(1, c, g1)

    def stage_back_corner(c):
        h_copies[c].wait_recv()
        answer(2, c, g2)

    stages = [stage_corner, stage_near, stage_own, stage_back_near, stage_back_corner]
    steps = [(c + 2 * i, i, c) for i in range(len(stages)) for c in range(chunks)]
    for _, i, c in sorted(steps):
        stages[i](c)

    for copy in b_copies.values():
        copy.wait_recv()

    for copy in locals_:
        copy.wait()
    for copy in sends:
        copy.wait_send()


def on_device(star_residual, patch_inverse, block_owner, block_slot, recv_target):
    nx, ny, nz = lax.axis_size("gx"), lax.axis_size("gy"), lax.axis_size("gz")
    patch_count, rhs_count, patch_order = star_residual.shape
    block_count = block_owner.shape[1]
    width = patch_order // block_count
    capacity = recv_target.shape[2]
    total = patch_count * block_count
    ly, lz = len(offsets(ny)), len(offsets(nz))
    count = ly * lz
    slots = count * 3 * capacity
    chunks = CHUNKS
    rows = rhs_count // chunks
    smem = pl.BlockSpec(memory_space=pltpu.SMEM)
    anywhere = pl.BlockSpec(memory_space=pl.ANY)
    f32 = jnp.float32
    slotted = pltpu.VMEM((chunks, slots, rows, width), f32)
    targeted = pltpu.VMEM((chunks, OWNB, rows, width), f32)
    dma = pltpu.SemaphoreType.DMA
    held, back = pl.pallas_call(
        functools.partial(kernel, (nx, ny, nz, chunks, block_count, capacity)),
        out_shape=(
            jax.ShapeDtypeStruct((OWNB, rhs_count, width), f32),
            jax.ShapeDtypeStruct((slots, rhs_count, width), f32),
        ),
        in_specs=[smem, smem, smem, anywhere, anywhere],
        out_specs=(anywhere, anywhere),
        scratch_shapes=[
            pltpu.VMEM(star_residual.shape, star_residual.dtype),
            pltpu.VMEM((total, width, patch_order), patch_inverse.dtype),
            pltpu.SMEM((total,), jnp.int32),
            pltpu.SMEM((slots,), jnp.int32),
            slotted, slotted,
            pltpu.VMEM((3, count * capacity, width), jnp.int32),
            pltpu.VMEM((3, count * capacity, width), jnp.int32),
            targeted, targeted, targeted, targeted, targeted, targeted, targeted,
            slotted,
            dma((chunks,)), dma((3, chunks)),
            dma((patch_count + 1,)), dma((2,)), dma((2,)),
            dma((count, 3, chunks)), dma((count, 3, chunks)),
            dma((chunks,)), dma((chunks,)), dma((chunks,)), dma((chunks,)),
            dma((chunks,)), dma((chunks,)), dma((chunks,)), dma((chunks,)),
            dma((count, 3, chunks)), dma((count, 3, chunks)),
        ],
        compiler_params=pltpu.CompilerParams(
            collective_id=0, has_side_effects=True, vmem_limit_bytes=56 * 1024 * 1024),
    )(block_owner, block_slot, recv_target.transpose(0, 2, 1), star_residual,
      patch_inverse.reshape(total, width, patch_order))
    return pl.pallas_call(
        functools.partial(gather_kernel, ((nx, ny, nz), capacity)),
        out_shape=(
            jax.ShapeDtypeStruct((OWNB, rhs_count, width), f32),
            jax.ShapeDtypeStruct((patch_count, block_count, rhs_count, width), f32),
        ),
        in_specs=[smem, smem, anywhere, anywhere],
        out_specs=(anywhere, anywhere),
        scratch_shapes=[
            pltpu.VMEM((OWNB, rhs_count, width), f32),
            pltpu.VMEM((patch_count, block_count, rhs_count, width), f32),
            dma((patch_count + 1,)), dma((patch_count + 1,)),
        ],
    )(block_owner, block_slot, held, back)


def solution(mesh):
    placed = (
        P(("gx", "gy", "gz"), None, None),
        P(("gx", "gy", "gz"), None, None),
        P(("gx", "gy", "gz"), None),
        P(("gx", "gy", "gz"), None),
        P(("gx", "gy", "gz"), None, None),
    )
    return jax.shard_map(
        on_device,
        mesh=mesh,
        in_specs=placed,
        out_specs=(P(("gx", "gy", "gz"), None, None), P(("gx", "gy", "gz"), None, None, None)),
        check_vma=False,
    )
```
